32 devices in a mesh: lat: 4 (over x, core), lon: 8 (over z, y).
Axes of the slice: x: 2, y: 2, z: 4, core: 2. Of those that a mesh axis runs over, the one named last changes fastest.
Arguments:
- tokens: bfloat16 [4, 56, 32, 1536], P(None, 'lat', 'lon'), may hold values from -400 to 400, as said below
- in_bounds: int32 [5], replicated, may hold values from 0 to 47, as said below
- out_bounds: int32 [5], replicated, may hold values from 0 to 24, as said below
- down_gain: float32 [768], replicated, may hold values from 0.25 to 1.75
- down_bias: float32 [768], replicated, may hold values from -1 to 1
- down_weight: bfloat16 [768, 384], replicated, may hold values from -0.21875 to 0.21875
- up_weight: bfloat16 [384, 768], replicated, may hold values from -0.3125 to 0.3125
- up_gain: float32 [192], replicated, may hold values from 0.25 to 1.75
- up_bias: float32 [192], replicated, may hold values from -1 to 1
- out_weight: bfloat16 [192, 192], replicated, may hold values from -0.4375 to 0.4375
Outputs:
- merged: bfloat16 [4, 32, 16, 3072], P(None, 'lat', 'lon')
- upsampled: bfloat16 [4, 56, 32, 1536], P(None, 'lat', 'lon')
The draws below stay inside these ranges and needn't reach their ends.
Inputs may be any that keep to these rules, and one draw needn't show every extreme that they name: `tokens`: band b's fine rows stand in its slots from the first one on; slots past the band's count hold values that no output reads. in_bounds[0] = 0, in_bounds[4] = 47; each band has 10 to 14 fine rows, and some band has 14. out_bounds[0] = 0, out_bounds[4] = 24; each band has 4 to 8 merged rows, and some band has 8. For 0 < b < 4, 2 * out_bounds[b] - in_bounds[b] is 1 to 3, and 3 for some b; so merged band b covers fine rows from band b's first on to at most 3 rows past its last (fine row 47 counting as zeros), and band b's fine rows need merged rows from at most 2 rows before merged band b's first up to its last, 2 being reached.
All inputs are finite; a program needn't handle non-finite values.
Results may differ from the reference program's by a relative error of at most 0.0069.
Values may be sent and summed in bfloat16 or wider, within the bound.
No kernel may reach another device: no remote copies, remote signals or barrier semaphores. Data moves between devices by JAX's collectives and lax.ppermute only.
A program may use at most 64 MiB of HBM per device.

```python
import math
import jax
import jax.numpy as jnp
from jax import lax

C = 192
LEV = 8
ROWS_DEV = 12
LON_DEV = 4
MEMBERS = 4
LCAP = 14
MCAP = 8
LAT = 47
MLAT = 24
LON = 32
N_LAT = 4
N_LON = 8


def pick_three(pattern, first, second, third):
    return jnp.where(pattern == 0, first, jnp.where(pattern == 1, second, third))


def bound_pair(key):
    base_key = jax.random.fold_in(key, 11)
    key_index, key_pattern, key_extra = jax.random.split(base_key, 3)
    places = jnp.arange(N_LAT + 1, dtype=jnp.int32)
    coarse_table = jnp.array([0, 1, 1, 1, 2], jnp.int32)
    fine_table = jnp.array([-1, -1, 0, 1, 1], jnp.int32)
    choose = jax.random.randint(key_index, (N_LAT + 1,), 0, 5).astype(jnp.int32)
    coarse_moves = jnp.take(coarse_table, choose)
    fine_moves = jnp.take(fine_table, choose)
    pattern = jax.random.randint(key_pattern, (), 0, 3).astype(jnp.int32)
    extra = jax.random.randint(key_extra, (), -1, 2).astype(jnp.int32)
    coarse_one = pick_three(pattern, 0, 2, coarse_moves[1])
    fine_one = pick_three(pattern, -1, 1, fine_moves[1])
    coarse_two = pick_three(pattern, 2, 0, 0)
    fine_two = pick_three(pattern, 1, -1, -1)
    coarse_three = pick_three(pattern, 1, jnp.where(extra > 0, 2, 1), 2)
    fine_three = pick_three(pattern, extra, 1, 1)
    coarse_moves = jnp.where(places == 1, coarse_one, jnp.where(places == 2, coarse_two, jnp.where(places == 3, coarse_three, coarse_moves)))
    fine_moves = jnp.where(places == 1, fine_one, jnp.where(places == 2, fine_two, jnp.where(places == 3, fine_three, fine_moves)))
    edges = (places == 0) | (places == N_LAT)
    fine_moves = jnp.where(edges, 0, fine_moves)
    coarse_moves = jnp.where(edges, 0, coarse_moves)
    fine_bounds = places * ROWS_DEV + fine_moves
    fine_bounds = jnp.where(places == N_LAT, N_LAT * ROWS_DEV - 1, fine_bounds)
    coarse_bounds = places * (ROWS_DEV // 2) + coarse_moves
    return (fine_bounds.astype(jnp.int32), coarse_bounds.astype(jnp.int32))


def draw_in_bounds(key, part):
    return bound_pair(key)[0]


def draw_out_bounds(key, part):
    return bound_pair(key)[1]


def draw_tokens(key, part):
    key_base, key_rows, key_chan = jax.random.split(jax.random.fold_in(key, 5), 3)
    shape = (MEMBERS, N_LAT * (ROWS_DEV + 2), LON_DEV * N_LON, LEV * C)
    row_scale = jnp.exp(jax.random.uniform(key_rows, (MEMBERS, N_LAT * (ROWS_DEV + 2), LON_DEV * N_LON, 1), jnp.float32, 0.0, math.log(10.0)))
    chan_scale = jnp.exp(jax.random.uniform(key_chan, (1, 1, 1, LEV * C), jnp.float32, 0.0, math.log(10.0)))
    values = jnp.clip(jax.random.normal(key_base, shape, jnp.float32), -4.0, 4.0)
    return (values * row_scale * chan_scale).astype(jnp.bfloat16)


def bell_draw(stream_key, shape, width, reach, kind=jnp.bfloat16):
    return jnp.clip(width * jax.random.normal(stream_key, shape, jnp.float32), -reach, reach).astype(kind)


def setup_inputs(seed: int = 0) -> dict:
    seeds = jax.random.split(jax.random.key(seed), 11)
    return {
        "tokens": draw_tokens(jax.random.fold_in(seeds[10], 71), 0),
        "in_bounds": draw_in_bounds(jax.random.fold_in(seeds[10], 71), 0),
        "out_bounds": draw_out_bounds(jax.random.fold_in(seeds[10], 71), 0),
        "down_gain": jnp.clip(1.0 + 0.15 * jax.random.normal(seeds[3], (4 * C,), jnp.float32), 0.25, 1.75),
        "down_bias": bell_draw(seeds[4], (4 * C,), 0.3, 1.0, jnp.float32),
        "down_weight": bell_draw(seeds[5], (4 * C, 2 * C), (4 * C) ** -0.5, 0.21875),
        "up_weight": bell_draw(seeds[6], (2 * C, 4 * C), (2 * C) ** -0.5, 0.3125),
        "up_gain": jnp.clip(1.0 + 0.15 * jax.random.normal(seeds[7], (C,), jnp.float32), 0.25, 1.75),
        "up_bias": bell_draw(seeds[8], (C,), 0.3, 1.0, jnp.float32),
        "out_weight": bell_draw(seeds[9], (C, C), C ** -0.5, 0.4375),
    }


def layer_norm(values, scale_vec, shift_vec):
    center = lax.optimization_barrier(jnp.mean(values, axis=-1, keepdims=True))
    spread = lax.optimization_barrier(jnp.mean(jnp.square(values - center), axis=-1, keepdims=True))
    return (values - center) * lax.rsqrt(spread + 1e-05) * scale_vec + shift_vec

def reference(tokens, in_bounds, out_bounds, down_gain, down_bias, down_weight, up_weight, up_gain, up_bias, out_weight):
    half_lon = LON // 2
    lat_rows = jnp.arange(LAT, dtype=jnp.int32)
    band_of = lax.optimization_barrier(jnp.sum((lat_rows[:, None] >= in_bounds[None, 1:N_LAT]).astype(jnp.int32), axis=1)).astype(jnp.int32)
    slot_of = (band_of * LCAP + lat_rows - in_bounds[band_of]).astype(jnp.int32)

    def one_member(member):
        token_grid = jnp.take(member, slot_of, axis=0)
        token_grid = jnp.concatenate([token_grid, jnp.zeros((1, LON, LEV * C), jnp.bfloat16)], axis=0)
        token_grid = jnp.roll(token_grid, 1, axis=1)
        pieces = token_grid.reshape(MLAT, 2, half_lon, 2, LEV, C).transpose(0, 2, 4, 3, 1, 5).reshape(-1, 4 * C)
        normed = layer_norm(pieces.astype(jnp.float32), down_gain, down_bias).astype(jnp.bfloat16)
        coarse = jnp.dot(normed, down_weight, preferred_element_type=jnp.float32).astype(jnp.bfloat16)
        widened = jnp.dot(coarse, up_weight, preferred_element_type=jnp.float32).astype(jnp.bfloat16)
        widened = widened.reshape(MLAT, half_lon, LEV, 2, 2, C).transpose(0, 4, 1, 3, 2, 5).reshape(2 * MLAT, LON, LEV, C)
        widened = jnp.roll(widened, -1, axis=1)[:LAT]
        renormed = layer_norm(widened.astype(jnp.float32), up_gain, up_bias).astype(jnp.bfloat16)
        finished = jnp.dot(renormed.reshape(-1, C), out_weight, preferred_element_type=jnp.float32).astype(jnp.bfloat16)
        return (coarse.reshape(MLAT, half_lon, LEV * 2 * C), finished.reshape(LAT, LON, LEV * C))
    coarse_all, fine_all = lax.map(one_member, tokens)
    fine_slots = jnp.arange(N_LAT * LCAP, dtype=jnp.int32)
    fine_band = (fine_slots // LCAP).astype(jnp.int32)
    fine_offset = (fine_slots % LCAP).astype(jnp.int32)
    fine_source = jnp.clip(in_bounds[fine_band] + fine_offset, 0, LAT - 1).astype(jnp.int32)
    fine_live = fine_offset < in_bounds[fine_band + 1] - in_bounds[fine_band]
    upsampled = jnp.where(fine_live[None, :, None, None], jnp.take(fine_all, fine_source, axis=1), jnp.zeros((), jnp.bfloat16))
    coarse_slots = jnp.arange(N_LAT * MCAP, dtype=jnp.int32)
    coarse_band = (coarse_slots // MCAP).astype(jnp.int32)
    coarse_offset = (coarse_slots % MCAP).astype(jnp.int32)
    coarse_source = jnp.clip(out_bounds[coarse_band] + coarse_offset, 0, MLAT - 1).astype(jnp.int32)
    coarse_live = coarse_offset < out_bounds[coarse_band + 1] - out_bounds[coarse_band]
    merged = jnp.where(coarse_live[None, :, None, None], jnp.take(coarse_all, coarse_source, axis=1), jnp.zeros((), jnp.bfloat16))
    return (merged.astype(jnp.bfloat16), upsampled.astype(jnp.bfloat16))
```

```python
import functools
import jax
import jax.numpy as jnp
from jax import lax
from jax.experimental import pallas as pl
from jax.experimental.pallas import tpu as pltpu
from jax.sharding import PartitionSpec as P

BELOW = 3
ABOVE = 1
BF = jnp.bfloat16
F32 = jnp.float32
I32 = jnp.int32


def up_to(n, m):
    return -(-n // m) * m


def column(rows):
    return lax.broadcasted_iota(I32, (rows, 1), 0)


def split(index, size, count):
    outer = jnp.zeros_like(index)
    for i in range(1, count):
        outer = outer + (index >= i * size).astype(I32)
    return outer, index - outer * size


def one_hot(target, width):
    lanes = lax.broadcasted_iota(I32, (target.shape[0], width), 1)
    return jnp.where(lanes == target, 1.0, 0.0).astype(F32).astype(BF)


def dot(a, b):
    return jnp.dot(a, b, preferred_element_type=F32)


def layer_norm(values, scale_vec, shift_vec):
    center = jnp.mean(values, axis=-1, keepdims=True)
    moved = values - center
    spread = jnp.mean(jnp.square(moved), axis=-1, keepdims=True)
    return moved * lax.rsqrt(spread + 1e-05) * scale_vec + shift_vec


class Sizes:
    def __init__(self, tokens, down_weight):
        self.members, self.slots, self.cols, self.packed = tokens.shape
        self.channels = down_weight.shape[0] // 4
        self.levels = self.packed // self.channels
        self.mslots = self.slots // 2 + 1
        self.mrows = self.mslots + 2
        self.mpad = up_to(self.members * self.mrows, 16)
        self.own = self.members * self.slots * self.cols
        self.below = self.members * BELOW * self.cols
        self.above = self.members * ABOVE * self.cols
        self.halo = self.members * (BELOW + ABOVE)


def bounds_of(in_ref, out_ref):
    band = lax.axis_index("lat")
    return in_ref[band], in_ref[band + 1], out_ref[band], out_ref[band + 1]


def wanted_rows(sz, start_in, side):
    member, k = split(column(sz.mpad), sz.mrows, sz.members + 1)
    wanted = 2 * (lax.shift_right_logical(start_in, 1) + k) + side
    return member, wanted, member < sz.members


def pack_kernel(sz, in_ref, x_ref, west_ref, east_ref, up_ref, down_ref):
    band = lax.axis_index("lat")
    count = in_ref[band + 1] - in_ref[band]
    n = sz.members * sz.slots
    ids = column(n)
    t_up = column(sz.below)
    member, rest = split(t_up, BELOW * sz.cols, sz.members)
    t_up = member * (sz.slots * sz.cols) + rest
    member, rest = split(column(sz.above), sz.cols, sz.members)
    t_down = member * (sz.slots * sz.cols) + (count - 1) * sz.cols + rest
    target = jnp.concatenate([ids * sz.cols, ids * sz.cols + sz.cols - 1, t_up, t_down], axis=0)
    x = x_ref[...].reshape(sz.own, sz.packed)
    out = dot(one_hot(target, sz.own), x)
    west_ref[...] = out[:n].astype(BF)
    east_ref[...] = out[n : 2 * n].astype(BF)
    up_ref[...] = out[2 * n : 2 * n + sz.below].astype(BF)
    down_ref[...] = out[2 * n + sz.below :].astype(BF)


def corner_kernel(sz, below_ref, above_ref, west_ref, east_ref):
    member, rest = split(column(sz.members * BELOW), BELOW, sz.members)
    t_below = (member * BELOW + rest) * sz.cols
    t_above = sz.below + column(sz.members * ABOVE) * sz.cols
    ids = jnp.concatenate([t_below, t_above], axis=0)
    target = jnp.concatenate([ids, ids + sz.cols - 1], axis=0)
    src = jnp.concatenate([below_ref[...], above_ref[...]], axis=0)
    out = dot(one_hot(target, sz.below + sz.above), src)
    west_ref[...] = out[: sz.halo].astype(BF)
    east_ref[...] = out[sz.halo :].astype(BF)


def merge(sz, groups, gain, bias, weight):
    parts = []
    c = sz.channels
    for level in range(sz.levels):
        lo = level * c
        for quad in groups:
            piece = jnp.concatenate([q[:, lo : lo + c] for q in quad], axis=1).astype(F32)
            parts.append(layer_norm(piece, gain, bias).astype(BF))
    return dot(jnp.concatenate(parts, axis=0), weight).astype(BF)


def finish(sz, block, gain, bias, weight):
    normed = layer_norm(block.astype(F32), gain, bias).astype(BF)
    return dot(normed, weight).astype(BF)


def by_lanes(sz, block, stride, offset):
    rows = [block[(lv * stride + offset) * sz.mpad : (lv * stride + offset + 1) * sz.mpad] for lv in range(sz.levels)]
    return jnp.concatenate(rows, axis=1)


def inner_kernel(sz, in_ref, out_ref, x_ref, below_ref, above_ref, dg, db, dw, uw, ug, ub, ow, gath_ref, merged_ref, fine_ref):
    start_in, end_in, _, _ = bounds_of(in_ref, out_ref)
    total = sz.own + sz.below + sz.above
    targets = []
    for x in range(sz.cols):
        for side in range(2):
            member, wanted, live = wanted_rows(sz, start_in, side)
            own = member * (sz.slots * sz.cols) + (wanted - start_in) * sz.cols + x
            low = sz.own + member * (BELOW * sz.cols) + (wanted - end_in) * sz.cols + x
            high = sz.own + sz.below + member * sz.cols + x
            t = jnp.where(wanted < start_in, high, jnp.where(wanted < end_in, own, low))
            targets.append(jnp.where(live & (wanted < end_in + BELOW), t, -1))
    hot = one_hot(jnp.concatenate(targets, axis=0), total)
    src = jnp.concatenate([x_ref[...].reshape(sz.own, sz.packed), below_ref[...], above_ref[...]], axis=0)
    gathered = dot(hot, src).astype(BF)
    two = 2 * sz.mpad
    gath_ref[:two] = gathered[:two]
    gath_ref[two:] = gathered[(sz.cols - 1) * two :]
    stage = [gathered[i * sz.mpad : (i + 1) * sz.mpad] for i in range(2, 2 * sz.cols - 2)]
    inner = sz.cols // 2 - 1
    groups = [stage[4 * i : 4 * i + 4] for i in range(inner)]
    coarse = merge(sz, groups, dg[...], db[...], dw[...])
    widened = dot(coarse, uw[...]).astype(BF)
    c = sz.channels
    done = [finish(sz, widened[:, b * c : (b + 1) * c], ug[...], ub[...], ow[...]) for b in range(4)]
    for i in range(inner):
        merged_ref[i * sz.mpad : (i + 1) * sz.mpad] = by_lanes(sz, coarse, inner, i)
        for b in range(4):
            at = (4 * i + b) * sz.mpad
            fine_ref[at : at + sz.mpad] = by_lanes(sz, done[b], inner, i)


def edge_kernel(sz, in_ref, out_ref, gath_ref, west_ref, wcorner_ref, east_ref, ecorner_ref, inm_ref, inf_ref, dg, db, dw, uw, ug, ub, ow, merged_ref, fine_ref):
    start_in, end_in, start_out, end_out = bounds_of(in_ref, out_ref)
    n = sz.members * sz.slots
    targets = []
    for side in range(2):
        member, wanted, live = wanted_rows(sz, start_in, side)
        own = member * sz.slots + (wanted - start_in)
        low = n + member * BELOW + (wanted - end_in)
        high = n + sz.members * BELOW + member
        t = jnp.where(wanted < start_in, high, jnp.where(wanted < end_in, own, low))
        targets.append(jnp.where(live & (wanted < end_in + BELOW), t, -1))
    hot = one_hot(jnp.concatenate(targets, axis=0), n + sz.halo)
    gw = dot(hot, jnp.concatenate([west_ref[...], wcorner_ref[...]], axis=0)).astype(BF)
    ge = dot(hot, jnp.concatenate([east_ref[...], ecorner_ref[...]], axis=0)).astype(BF)
    mp = sz.mpad
    groups = [
        [gw[:mp], gw[mp:], gath_ref[:mp], gath_ref[mp : 2 * mp]],
        [gath_ref[2 * mp : 3 * mp], gath_ref[3 * mp :], ge[:mp], ge[mp:]],
    ]
    c = sz.channels
    finer = [[], []]
    coarse = merge(sz, groups[:1], dg[...], db[...], dw[...])
    right = merge(sz, groups[1:], dg[...], db[...], dw[...])
    wide_left = dot(coarse, uw[:, 2 * c :]).astype(BF)
    wide_right = dot(right, uw[:, : 2 * c]).astype(BF)
    finer = [
        by_lanes(sz, finish(sz, wide[:, a * c : (a + 1) * c], ug[...], ub[...], ow[...]), 1, 0)
        for wide in (wide_left, wide_right)
        for a in range(2)
    ]
    first = lax.shift_right_logical(start_in, 1)
    half = sz.cols // 2
    rows = column(sz.members * sz.mslots * half)
    member, rest = split(rows, sz.mslots * half, sz.members)
    slot, j = split(rest, half, sz.mslots)
    t = j * mp + member * sz.mrows + slot + (start_out - first)
    t = jnp.where(slot < end_out - start_out, t, -1)
    src = jnp.concatenate([by_lanes(sz, coarse, 1, 0), inm_ref[...]], axis=0)
    merged = dot(one_hot(t, half * mp), src).astype(BF)
    merged_ref[...] = merged.reshape(merged_ref.shape)
    rows = column(sz.own)
    member, rest = split(rows, sz.slots * sz.cols, sz.members)
    slot, x = split(rest, sz.cols, sz.slots)
    row = start_in + slot
    k = lax.shift_right_logical(row, 1)
    t = (2 * x + (row - 2 * k)) * mp + member * sz.mrows + (k - first)
    t = jnp.where(slot < end_in - start_in, t, -1)
    src = jnp.concatenate(finer[:2] + [inf_ref[...]] + finer[2:], axis=0)
    fine = dot(one_hot(t, 2 * sz.cols * mp), src).astype(BF)
    fine_ref[...] = fine.reshape(fine_ref.shape)


def call(kernel, name, args, outs, smem):
    spec_s = pl.BlockSpec(memory_space=pltpu.SMEM)
    spec_v = pl.BlockSpec(memory_space=pltpu.VMEM)
    return pl.pallas_call(
        kernel,
        name=name,
        in_specs=[spec_s] * smem + [spec_v] * (len(args) - smem),
        out_specs=[spec_v] * len(outs),
        out_shape=[jax.ShapeDtypeStruct(s, BF) for s in outs],
    )(*args)


def along(value, axis, steps, ring):
    size = lax.axis_size(axis)
    pairs = [(i, (i + steps) % size) for i in range(size) if ring or 0 <= i + steps < size]
    return lax.ppermute(value, axis, pairs)


def body(tokens, in_bounds, out_bounds, down_gain, down_bias, down_weight, up_weight, up_gain, up_bias, out_weight):
    sz = Sizes(tokens, down_weight)
    n = sz.members * sz.slots
    x = tokens.reshape(n, sz.cols, sz.packed)
    params = (
        down_gain.reshape(1, -1),
        down_bias.reshape(1, -1),
        down_weight,
        up_weight,
        up_gain.reshape(1, -1),
        up_bias.reshape(1, -1),
        out_weight,
    )
    p = sz.packed
    west, east, up, down = call(
        functools.partial(pack_kernel, sz), "pack", (in_bounds, x), [(n, p), (n, p), (sz.below, p), (sz.above, p)], 1
    )
    below = along(up, "lat", -1, False)
    above = along(down, "lat", 1, False)
    from_west = along(east, "lon", 1, True)
    from_east = along(west, "lon", -1, True)
    cwest, ceast = call(functools.partial(corner_kernel, sz), "corner", (below, above), [(sz.halo, p)] * 2, 0)
    corner_west = along(ceast, "lon", 1, True)
    corner_east = along(cwest, "lon", -1, True)
    inner = sz.cols // 2 - 1
    gath, in_merged, in_fine = call(
        functools.partial(inner_kernel, sz),
        "inner",
        (in_bounds, out_bounds, x, below, above) + params,
        [(4 * sz.mpad, p), (inner * sz.mpad, 2 * p), (4 * inner * sz.mpad, p)],
        2,
    )
    merged, fine = call(
        functools.partial(edge_kernel, sz),
        "edge",
        (in_bounds, out_bounds, gath, from_west, corner_west, from_east, corner_east, in_merged, in_fine) + params,
        [(sz.members * sz.mslots, sz.cols // 2, 2 * p), (n, sz.cols, p)],
        2,
    )
    return (
        merged.reshape(sz.members, sz.mslots, sz.cols // 2, 2 * p),
        fine.reshape(sz.members, sz.slots, sz.cols, p),
    )


def solution(mesh):
    return jax.shard_map(
        body,
        mesh=mesh,
        in_specs=(P(None, "lat", "lon", None),) + (P(),) * 9,
        out_specs=(P(None, "lat", "lon", None), P(None, "lat", "lon", None)),
        check_vma=False,
    )
```

```python
import functools
import jax
import jax.numpy as jnp
from jax import lax
from jax.experimental import pallas as pl
from jax.experimental.pallas import tpu as pltpu
from jax.sharding import PartitionSpec as P

HALO = 3
BF = jnp.bfloat16
F32 = jnp.float32
I32 = jnp.int32


def up_to(n, m):
    return -(-n // m) * m


def column(rows):
    return lax.broadcasted_iota(I32, (rows, 1), 0)


def split(index, size, count):
    outer = jnp.zeros_like(index)
    for i in range(1, count):
        outer = outer + (index >= i * size).astype(I32)
    return outer, index - outer * size


def one_hot(target, width):
    lanes = lax.broadcasted_iota(I32, (target.shape[0], width), 1)
    return jnp.where(lanes == target, 1.0, 0.0).astype(F32).astype(BF)


def dot(a, b):
    return jnp.dot(a, b, preferred_element_type=F32)


def layer_norm(values, scale_vec, shift_vec):
    center = jnp.mean(values, axis=-1, keepdims=True)
    moved = values - center
    spread = jnp.mean(jnp.square(moved), axis=-1, keepdims=True)
    return moved * lax.rsqrt(spread + 1e-05) * scale_vec + shift_vec


class Sizes:
    def __init__(self, tokens, down_weight):
        self.members, self.slots, self.cols, self.packed = tokens.shape
        self.channels = down_weight.shape[0] // 4
        self.levels = self.packed // self.channels
        self.mslots = self.slots // 2 + 1
        self.mrows = self.mslots + 2
        self.mp = up_to(self.members * self.mrows, 8)
        self.own = self.members * self.slots * self.cols
        self.halo = self.members * HALO * self.cols
        self.half = self.cols // 2


def bounds_of(in_ref, out_ref):
    band = lax.axis_index("lat")
    return in_ref[band], in_ref[band + 1], out_ref[band], out_ref[band + 1]


def even(axis):
    return 1 - lax.rem(lax.axis_index(axis), 2)


def fetch(pairs, sems):
    copies = [pltpu.make_async_copy(a, b, sems.at[i]) for i, (a, b) in enumerate(pairs)]
    for copy in copies:
        copy.start()
    return copies


def rows_kernel(sz, in_ref, x_ref, a_ref, b_ref, sems):
    band = lax.axis_index("lat")
    last = in_ref[band + 1] - in_ref[band] - HALO
    first = even("lat") * last
    pairs = [(x_ref.at[:, pl.ds(first, HALO)], a_ref), (x_ref.at[:, pl.ds(last - first, HALO)], b_ref)]
    for copy in fetch(pairs, sems):
        copy.wait()


def gather_kernel(sz, in_ref, x_ref, a_ref, b_ref, send_a, send_b, inner_ref):
    band = lax.axis_index("lat")
    start_in, end_in = in_ref[band], in_ref[band + 1]
    below = sz.own + (1 - even("lat")) * sz.halo
    above = sz.own + even("lat") * sz.halo
    step = HALO * sz.cols
    far = (sz.cols - 1) * even("lon")
    member, k = split(column(sz.mp), sz.mrows, sz.members + 1)
    targets = []
    for x in [far, sz.cols - 1 - far] + list(range(1, sz.cols - 1)):
        for side in range(2):
            wanted = 2 * (lax.shift_right_logical(start_in, 1) + k) + side
            own = member * (sz.slots * sz.cols) + (wanted - start_in) * sz.cols + x
            low = below + member * step + (wanted - end_in) * sz.cols + x
            high = above + member * step + (HALO - 1) * sz.cols + x
            t = jnp.where(wanted < start_in, high, jnp.where(wanted < end_in, own, low))
            targets.append(jnp.where((member < sz.members) & (wanted < end_in + HALO), t, -1))
    hot = one_hot(jnp.concatenate(targets, axis=0), sz.own + 2 * sz.halo)
    src = [x_ref[...].reshape(sz.own, sz.packed)]
    src += [r[...].reshape(sz.halo, sz.packed) for r in (a_ref, b_ref)]
    out = dot(hot, jnp.concatenate(src, axis=0)).astype(BF)
    two = 2 * sz.mp
    send_a[...] = out[:two]
    send_b[...] = out[two : 2 * two]
    inner_ref[...] = out[2 * two :]


def merge(sz, columns, gain, bias, weight):
    parts = []
    c = sz.channels
    for level in range(sz.levels):
        for quad in columns:
            at = slice(level * c, level * c + c)
            piece = jnp.concatenate([q[:, at] for q in quad], axis=1)
            parts.append(layer_norm(piece, gain, bias))
    return dot(jnp.concatenate(parts, axis=0).astype(BF), weight)


def finish(sz, block, gain, bias, weight):
    normed = layer_norm(block, gain, bias).astype(BF)
    return dot(normed, weight)


def by_lanes(sz, block, stride, offset):
    rows = [block[(lv * stride + offset) * sz.mp : (lv * stride + offset + 1) * sz.mp] for lv in range(sz.levels)]
    return jnp.concatenate(rows, axis=1)


def halves(sz, block):
    block = block.astype(F32)
    return [block[: sz.mp], block[sz.mp :]]


def row(ref):
    return ref[...].reshape(1, -1)


def inner_kernel(sz, p_ref, dg, db, dw_ref, uw_ref, ug, ub, ow_ref, merged_ref, fine_ref, dw, uw, ow, sems):
    copies = fetch([(dw_ref, dw), (uw_ref, uw), (ow_ref, ow)], sems)
    inner = sz.half - 1
    two = 2 * sz.mp
    columns = []
    for i in range(inner):
        quad = []
        for j in range(2):
            quad += halves(sz, p_ref[(2 * i + j) * two : (2 * i + j + 1) * two])
        columns.append(quad)
    copies[0].wait()
    coarse = merge(sz, columns, row(dg), row(db), dw[...])
    copies[1].wait()
    widened = dot(coarse.astype(BF), uw[...]).astype(BF).astype(F32)
    copies[2].wait()
    c = sz.channels
    done = [finish(sz, widened[:, b * c : (b + 1) * c], row(ug), row(ub), ow[...]) for b in range(4)]
    merged = [by_lanes(sz, coarse, inner, i) for i in range(inner)]
    merged_ref[...] = jnp.concatenate(merged, axis=0).astype(BF)
    fine = [by_lanes(sz, done[b], inner, i) for i in range(inner) for b in range(4)]
    fine_ref[...] = jnp.concatenate(fine, axis=0).astype(BF)


def edge_kernel(
    sz, in_ref, out_ref, own_a, own_b, got_a_ref, got_b_ref, dg, db, dw_ref, uw_ref, ug, ub, ow_ref, inm_ref, inf_ref,
    merged_ref, fine_ref, oa, ob, ga, gb, dw, uw, ow, inm, inf, sems,
):
    copies = fetch(
        [(own_a, oa), (own_b, ob), (got_a_ref, ga), (got_b_ref, gb), (dw_ref, dw), (uw_ref, uw), (ow_ref, ow), (inm_ref, inm), (inf_ref, inf)],
        sems,
    )
    start_in, end_in, start_out, end_out = bounds_of(in_ref, out_ref)
    is_even = even("lon") == 1
    mp = sz.mp
    c = sz.channels
    first = lax.shift_right_logical(start_in, 1)
    rows = column(sz.members * sz.mslots * sz.half)
    member, rest = split(rows, sz.mslots * sz.half, sz.members)
    slot, j = split(rest, sz.half, sz.mslots)
    t = j * mp + member * sz.mrows + slot + (start_out - first)
    merged_hot = one_hot(jnp.where(slot < end_out - start_out, t, -1), sz.half * mp)
    rows = column(sz.own)
    member, rest = split(rows, sz.slots * sz.cols, sz.members)
    slot, x = split(rest, sz.cols, sz.slots)
    at = start_in + slot
    k = lax.shift_right_logical(at, 1)
    t = (2 * x + (at - 2 * k)) * mp + member * sz.mrows + (k - first)
    fine_hot = one_hot(jnp.where(slot < end_in - start_in, t, -1), 2 * sz.cols * mp)
    for copy in copies[:4]:
        copy.wait()
    a, b, ra, rb = oa[...], ob[...], ga[...], gb[...]
    left = halves(sz, jnp.where(is_even, rb, ra)) + halves(sz, jnp.where(is_even, b, a))
    right = halves(sz, jnp.where(is_even, a, b)) + halves(sz, jnp.where(is_even, ra, rb))
    copies[4].wait()
    coarse_left = merge(sz, [left], row(dg), row(db), dw[...])
    coarse_right = merge(sz, [right], row(dg), row(db), dw[...])
    copies[5].wait()
    wide_left = dot(coarse_left.astype(BF), uw[:, 2 * c :]).astype(BF).astype(F32)
    wide_right = dot(coarse_right.astype(BF), uw[:, : 2 * c]).astype(BF).astype(F32)
    for copy in copies[6:]:
        copy.wait()
    finer = [
        by_lanes(sz, finish(sz, wide[:, s * c : (s + 1) * c], row(ug), row(ub), ow[...]), 1, 0)
        for wide in (wide_left, wide_right)
        for s in range(2)
    ]
    src = jnp.concatenate([by_lanes(sz, coarse_left, 1, 0), inm[...].astype(F32)], axis=0).astype(BF)
    merged_ref[...] = dot(merged_hot, src).astype(BF).reshape(merged_ref.shape)
    src = jnp.concatenate(finer[:2] + [inf[...].astype(F32)] + finer[2:], axis=0).astype(BF)
    fine_ref[...] = dot(fine_hot, src).astype(BF).reshape(fine_ref.shape)


ANY = pl.BlockSpec(memory_space=pl.ANY)
SM = pl.BlockSpec(memory_space=pltpu.SMEM)
VM = pl.BlockSpec(memory_space=pltpu.VMEM)


def call(kernel, name, args, specs, outs, out_spec, scratch=()):
    scratch = [pltpu.VMEM(a.shape, a.dtype) for a in scratch]
    sems = {"gather": 0, "rows": 2}.get(name, len(scratch))
    return pl.pallas_call(
        kernel,
        name=name,
        in_specs=specs,
        out_specs=[out_spec] * len(outs),
        out_shape=[jax.ShapeDtypeStruct(s, BF) for s in outs],
        scratch_shapes=scratch + ([pltpu.SemaphoreType.DMA((sems,))] if sems else []),
    )(*args)


def pair_swaps(first, second, axis, ring):
    size = lax.axis_size(axis)
    assert size % 2 == 0
    near = [(i, i ^ 1) for i in range(size)]
    far = [(i, i + 1 if i % 2 else i - 1) for i in range(size)]
    far = [(i, j % size) for i, j in far if ring or 0 <= j < size]
    return lax.ppermute(first, axis, near), lax.ppermute(second, axis, far)


def body(tokens, in_bounds, out_bounds, down_gain, down_bias, down_weight, up_weight, up_gain, up_bias, out_weight):
    sz = Sizes(tokens, down_weight)
    n = sz.members * sz.slots
    p = sz.packed
    part = functools.partial
    params = (down_gain, down_bias, down_weight, up_weight, up_gain, up_bias, out_weight)
    pspecs = [VM, VM, ANY, ANY, VM, VM, ANY]
    weights = [down_weight, up_weight, out_weight]
    lat_shape = (sz.members, HALO, sz.cols, p)
    row_a, row_b = call(part(rows_kernel, sz), "rows", (in_bounds, tokens), [SM, ANY], [lat_shape] * 2, ANY)
    row_a, row_b = pair_swaps(row_a, row_b, "lat", False)
    flat = [v.reshape(-1, sz.cols, p) for v in (tokens, row_a, row_b)]
    two = 2 * sz.mp
    inner = sz.half - 1
    send_a, send_b, mid = call(
        part(gather_kernel, sz), "gather", (in_bounds, *flat), [SM, VM, VM, VM], [(two, p), (two, p), (2 * inner * two, p)], VM
    )
    got_a, got_b = pair_swaps(send_a, send_b, "lon", True)
    in_merged, in_fine = call(
        part(inner_kernel, sz), "inner", (mid,) + params, [VM] + pspecs, [(inner * sz.mp, 2 * p), (4 * inner * sz.mp, p)], VM, weights
    )
    merged, fine = call(
        part(edge_kernel, sz),
        "edge",
        (in_bounds, out_bounds, send_a, send_b, got_a, got_b) + params + (in_merged, in_fine),
        [SM, SM, ANY, ANY, ANY, ANY] + pspecs + [ANY, ANY],
        [(sz.members * sz.mslots, sz.half, 2 * p), (n, sz.cols, p)],
        VM,
        [send_a, send_b, got_a, got_b] + weights + [in_merged, in_fine],
    )
    return (
        merged.reshape(sz.members, sz.mslots, sz.half, 2 * p),
        fine.reshape(sz.members, sz.slots, sz.cols, p),
    )


def solution(mesh):
    return jax.shard_map(
        body,
        mesh=mesh,
        in_specs=(P(None, "lat", "lon", None),) + (P(),) * 9,
        out_specs=(P(None, "lat", "lon", None), P(None, "lat", "lon", None)),
        check_vma=False,
    )
```

```python
import functools
import jax
import jax.numpy as jnp
from jax import lax
from jax.experimental import pallas as pl
from jax.experimental.pallas import tpu as pltpu
from jax.sharding import PartitionSpec as P

HALO = 3
BF = jnp.bfloat16
F32 = jnp.float32
I32 = jnp.int32


def up_to(n, m):
    return -(-n // m) * m


def column(rows):
    return lax.broadcasted_iota(I32, (rows, 1), 0)


def split(index, size, count):
    outer = jnp.zeros_like(index)
    for i in range(1, count):
        outer = outer + (index >= i * size).astype(I32)
    return outer, index - outer * size


def one_hot(target, width):
    lanes = lax.broadcasted_iota(I32, (target.shape[0], width), 1)
    return jnp.where(lanes == target, 1.0, 0.0).astype(F32).astype(BF)


def dot(a, b):
    return jnp.dot(a, b, preferred_element_type=F32)


def layer_norm(values, scale_vec, shift_vec):
    center = jnp.mean(values, axis=-1, keepdims=True)
    moved = values - center
    spread = jnp.mean(jnp.square(moved), axis=-1, keepdims=True)
    return moved * lax.rsqrt(spread + 1e-05) * scale_vec + shift_vec


class Sizes:
    def __init__(self, tokens, down_weight):
        self.members, self.slots, self.cols, self.packed = tokens.shape
        self.channels = down_weight.shape[0] // 4
        self.levels = self.packed // self.channels
        self.mslots = self.slots // 2 + 1
        self.mrows = self.mslots + 2
        self.mp = up_to(self.members * self.mrows, 8)
        self.own = self.members * self.slots * self.cols
        self.halo = self.members * HALO * self.cols
        self.half = self.cols // 2


def bounds_of(in_ref, out_ref):
    band = lax.axis_index("lat")
    return in_ref[band], in_ref[band + 1], out_ref[band], out_ref[band + 1]


def even(axis):
    return 1 - lax.rem(lax.axis_index(axis), 2)


def fetch(pairs, sems):
    copies = [pltpu.make_async_copy(a, b, sems.at[i]) for i, (a, b) in enumerate(pairs)]
    for copy in copies:
        copy.start()
    return copies


def rows_kernel(sz, in_ref, x_ref, a_ref, b_ref, sems):
    band = lax.axis_index("lat")
    last = in_ref[band + 1] - in_ref[band] - HALO
    first = even("lat") * last
    pairs = [(x_ref.at[:, pl.ds(first, HALO)], a_ref), (x_ref.at[:, pl.ds(last - first, HALO)], b_ref)]
    for copy in fetch(pairs, sems):
        copy.wait()


def gather_kernel(sz, in_ref, x_ref, a_ref, b_ref, send_a, send_b, inner_ref):
    band = lax.axis_index("lat")
    start_in, end_in = in_ref[band], in_ref[band + 1]
    below = sz.own + (1 - even("lat")) * sz.halo
    above = sz.own + even("lat") * sz.halo
    step = HALO * sz.cols
    far = (sz.cols - 1) * even("lon")
    member, k = split(column(sz.mp), sz.mrows, sz.members + 1)
    targets = []
    for x in [far, sz.cols - 1 - far] + list(range(1, sz.cols - 1)):
        for side in range(2):
            wanted = 2 * (lax.shift_right_logical(start_in, 1) + k) + side
            own = member * (sz.slots * sz.cols) + (wanted - start_in) * sz.cols + x
            low = below + member * step + (wanted - end_in) * sz.cols + x
            high = above + member * step + (HALO - 1) * sz.cols + x
            t = jnp.where(wanted < start_in, high, jnp.where(wanted < end_in, own, low))
            targets.append(jnp.where((member < sz.members) & (wanted < end_in + HALO), t, -1))
    hot = one_hot(jnp.concatenate(targets, axis=0), sz.own + 2 * sz.halo)
    src = [x_ref[...].reshape(sz.own, sz.packed)]
    src += [r[...].reshape(sz.halo, sz.packed) for r in (a_ref, b_ref)]
    out = dot(hot, jnp.concatenate(src, axis=0)).astype(BF)
    two = 2 * sz.mp
    send_a[...] = out[:two]
    send_b[...] = out[two : 2 * two]
    inner_ref[...] = out[2 * two :]


def merge(sz, columns, gain, bias, weight):
    parts = []
    c = sz.channels
    for level in range(sz.levels):
        for quad in columns:
            at = slice(level * c, level * c + c)
            piece = jnp.concatenate([q[:, at] for q in quad], axis=1)
            parts.append(layer_norm(piece, gain, bias))
    return dot(jnp.concatenate(parts, axis=0).astype(BF), weight)


def finish(sz, block, gain, bias, weight):
    normed = layer_norm(block, gain, bias).astype(BF)
    return dot(normed, weight)


def by_lanes(sz, block, stride, offset):
    rows = [block[(lv * stride + offset) * sz.mp : (lv * stride + offset + 1) * sz.mp] for lv in range(sz.levels)]
    return jnp.concatenate(rows, axis=1)


def halves(sz, block):
    block = block.astype(F32)
    return [block[: sz.mp], block[sz.mp :]]


def row(ref):
    return ref[...].reshape(1, -1)


def inner_kernel(sz, p_ref, dg, db, dw_ref, uw_ref, ug, ub, ow_ref, merged_ref, fine_ref, dw, uw, ow, sems):
    copies = fetch([(dw_ref, dw), (uw_ref, uw), (ow_ref, ow)], sems)
    inner = sz.half - 1
    two = 2 * sz.mp
    columns = []
    for i in range(inner):
        quad = []
        for j in range(2):
            quad += halves(sz, p_ref[(2 * i + j) * two : (2 * i + j + 1) * two])
        columns.append(quad)
    copies[0].wait()
    coarse = merge(sz, columns, row(dg), row(db), dw[...])
    copies[1].wait()
    widened = dot(coarse.astype(BF), uw[...]).astype(BF).astype(F32)
    copies[2].wait()
    c = sz.channels
    done = [finish(sz, widened[:, b * c : (b + 1) * c], row(ug), row(ub), ow[...]) for b in range(4)]
    merged = [by_lanes(sz, coarse, inner, i) for i in range(inner)]
    merged_ref[...] = jnp.concatenate(merged, axis=0).astype(BF)
    fine = [by_lanes(sz, done[b], inner, i) for i in range(inner) for b in range(4)]
    fine_ref[...] = jnp.concatenate(fine, axis=0).astype(BF)


def edge_kernel(
    sz, in_ref, out_ref, own_a, own_b, got_a_ref, got_b_ref, dg, db, dw_ref, uw_ref, ug, ub, ow_ref, inm_ref, inf_ref,
    merged_ref, fine_ref, oa, ob, ga, gb, dw, uw, ow, inm, inf, sems,
):
    copies = fetch(
        [(own_a, oa), (own_b, ob), (got_a_ref, ga), (got_b_ref, gb), (dw_ref, dw), (uw_ref, uw), (ow_ref, ow), (inm_ref, inm), (inf_ref, inf)],
        sems,
    )
    start_in, end_in, start_out, end_out = bounds_of(in_ref, out_ref)
    is_even = even("lon") == 1
    mp = sz.mp
    c = sz.channels
    first = lax.shift_right_logical(start_in, 1)
    rows = column(sz.members * sz.mslots * sz.half)
    member, rest = split(rows, sz.mslots * sz.half, sz.members)
    slot, j = split(rest, sz.half, sz.mslots)
    t = j * mp + member * sz.mrows + slot + (start_out - first)
    merged_hot = one_hot(jnp.where(slot < end_out - start_out, t, -1), sz.half * mp)
    rows = column(sz.own)
    member, rest = split(rows, sz.slots * sz.cols, sz.members)
    slot, x = split(rest, sz.cols, sz.slots)
    at = start_in + slot
    k = lax.shift_right_logical(at, 1)
    t = (2 * x + (at - 2 * k)) * mp + member * sz.mrows + (k - first)
    fine_hot = one_hot(jnp.where(slot < end_in - start_in, t, -1), 2 * sz.cols * mp)
    for copy in copies[:4]:
        copy.wait()
    a, b, ra, rb = oa[...], ob[...], ga[...], gb[...]
    left = halves(sz, jnp.where(is_even, rb, ra)) + halves(sz, jnp.where(is_even, b, a))
    right = halves(sz, jnp.where(is_even, a, b)) + halves(sz, jnp.where(is_even, ra, rb))
    copies[4].wait()
    coarse_left = merge(sz, [left], row(dg), row(db), dw[...])
    coarse_right = merge(sz, [right], row(dg), row(db), dw[...])
    copies[5].wait()
    wide_left = dot(coarse_left.astype(BF), uw[:, 2 * c :]).astype(BF).astype(F32)
    wide_right = dot(coarse_right.astype(BF), uw[:, : 2 * c]).astype(BF).astype(F32)
    for copy in copies[6:]:
        copy.wait()
    finer = [
        by_lanes(sz, finish(sz, wide[:, s * c : (s + 1) * c], row(ug), row(ub), ow[...]), 1, 0)
        for wide in (wide_left, wide_right)
        for s in range(2)
    ]
    src = jnp.concatenate([by_lanes(sz, coarse_left, 1, 0), inm[...].astype(F32)], axis=0).astype(BF)
    merged_ref[...] = dot(merged_hot, src).astype(BF).reshape(merged_ref.shape)
    src = jnp.concatenate(finer[:2] + [inf[...].astype(F32)] + finer[2:], axis=0).astype(BF)
    fine_ref[...] = dot(fine_hot, src).astype(BF).reshape(fine_ref.shape)


ANY = pl.BlockSpec(memory_space=pl.ANY)
SM = pl.BlockSpec(memory_space=pltpu.SMEM)
VM = pl.BlockSpec(memory_space=pltpu.VMEM)


def call(kernel, name, args, specs, outs, out_spec, scratch=()):
    scratch = [pltpu.VMEM(a.shape, a.dtype) for a in scratch]
    sems = {"gather": 0, "rows": 2}.get(name, len(scratch))
    return pl.pallas_call(
        kernel,
        name=name,
        in_specs=specs,
        out_specs=[out_spec] * len(outs),
        out_shape=[jax.ShapeDtypeStruct(s, BF) for s in outs],
        scratch_shapes=scratch + ([pltpu.SemaphoreType.DMA((sems,))] if sems else []),
    )(*args)


def pair_swaps(first, second, axis, ring):
    size = lax.axis_size(axis)
    assert size % 2 == 0
    near = [(i, i ^ 1) for i in range(size)]
    far = [(i, i + 1 if i % 2 else i - 1) for i in range(size)]
    far = [(i, j % size) for i, j in far if ring or 0 <= j < size]
    return lax.ppermute(first, axis, near), lax.ppermute(second, axis, far)


def body(tokens, in_bounds, out_bounds, down_gain, down_bias, down_weight, up_weight, up_gain, up_bias, out_weight):
    sz = Sizes(tokens, down_weight)
    n = sz.members * sz.slots
    p = sz.packed
    part = functools.partial
    params = (down_gain, down_bias, down_weight, up_weight, up_gain, up_bias, out_weight)
    pspecs = [VM, VM, ANY, ANY, VM, VM, ANY]
    weights = [down_weight, up_weight, out_weight]
    lat_shape = (sz.members, HALO, sz.cols, p)
    row_a, row_b = call(part(rows_kernel, sz), "rows", (in_bounds, tokens), [SM, ANY], [lat_shape] * 2, VM)
    row_a, row_b = pair_swaps(row_a, row_b, "lat", False)
    flat = [v.reshape(-1, sz.cols, p) for v in (tokens, row_a, row_b)]
    two = 2 * sz.mp
    inner = sz.half - 1
    send_a, send_b, mid = call(
        part(gather_kernel, sz), "gather", (in_bounds, *flat), [SM, VM, VM, VM], [(two, p), (two, p), (2 * inner * two, p)], VM
    )
    got_a, got_b = pair_swaps(send_a, send_b, "lon", True)
    in_merged, in_fine = call(
        part(inner_kernel, sz), "inner", (mid,) + params, [VM] + pspecs, [(inner * sz.mp, 2 * p), (4 * inner * sz.mp, p)], VM, weights
    )
    merged, fine = call(
        part(edge_kernel, sz),
        "edge",
        (in_bounds, out_bounds, send_a, send_b, got_a, got_b) + params + (in_merged, in_fine),
        [SM, SM, ANY, ANY, ANY, ANY] + pspecs + [ANY, ANY],
        [(sz.members * sz.mslots, sz.half, 2 * p), (n, sz.cols, p)],
        VM,
        [send_a, send_b, got_a, got_b] + weights + [in_merged, in_fine],
    )
    return (
        merged.reshape(sz.members, sz.mslots, sz.half, 2 * p),
        fine.reshape(sz.members, sz.slots, sz.cols, p),
    )


def solution(mesh):
    return jax.shard_map(
        body,
        mesh=mesh,
        in_specs=(P(None, "lat", "lon", None),) + (P(),) * 9,
        out_specs=(P(None, "lat", "lon", None), P(None, "lat", "lon", None)),
        check_vma=False,
    )
```

```python
import functools
import jax
import jax.numpy as jnp
from jax import lax
from jax.experimental import pallas as pl
from jax.experimental.pallas import tpu as pltpu
from jax.sharding import PartitionSpec as P

HALO = 3
CUT = 4
BF = jnp.bfloat16
F32 = jnp.float32
I32 = jnp.int32


def up_to(n, m):
    return -(-n // m) * m


def column(rows):
    return lax.broadcasted_iota(I32, (rows, 1), 0)


def split(index, size, count):
    outer = jnp.zeros_like(index)
    for i in range(1, count):
        outer = outer + (index >= i * size).astype(I32)
    return outer, index - outer * size


def one_hot(target, width):
    lanes = lax.broadcasted_iota(I32, (target.shape[0], width), 1)
    return jnp.where(lanes == target, 1.0, 0.0).astype(F32).astype(BF)


def dot(a, b):
    return jnp.dot(a, b, preferred_element_type=F32)


def layer_norm(values, scale_vec, shift_vec):
    center = jnp.mean(values, axis=-1, keepdims=True)
    moved = values - center
    spread = jnp.mean(jnp.square(moved), axis=-1, keepdims=True)
    return moved * lax.rsqrt(spread + 1e-05) * scale_vec + shift_vec


class Sizes:
    def __init__(self, tokens, down_weight):
        self.members, self.slots, self.cols, self.packed = tokens.shape
        self.channels = down_weight.shape[0] // 4
        self.levels = self.packed // self.channels
        self.mslots = self.slots // 2 + 1
        self.mrows = self.mslots + 2
        self.mp = up_to(self.members * self.mrows, 8)
        self.own = self.members * self.slots * self.cols
        self.halo = self.members * HALO * self.cols
        self.half = self.cols // 2


def bounds_of(in_ref, out_ref):
    band = lax.axis_index("lat")
    return in_ref[band], in_ref[band + 1], out_ref[band], out_ref[band + 1]


def even(axis):
    return 1 - lax.rem(lax.axis_index(axis), 2)


def fetch(pairs, sems):
    copies = [pltpu.make_async_copy(a, b, sems.at[i]) for i, (a, b) in enumerate(pairs)]
    for copy in copies:
        copy.start()
    return copies


def chunks(pair, count):
    size = pair[0].shape[0] // count
    return [(pair[0].at[i * size : (i + 1) * size], pair[1].at[i * size : (i + 1) * size]) for i in range(count)]


def finish_all(copies):
    for copy in copies:
        copy.wait()


def rows_kernel(sz, in_ref, x_ref, a_ref, b_ref, sems):
    band = lax.axis_index("lat")
    last = in_ref[band + 1] - in_ref[band] - HALO
    first = even("lat") * last
    pairs = [(x_ref.at[:, pl.ds(first, HALO)], a_ref), (x_ref.at[:, pl.ds(last - first, HALO)], b_ref)]
    for copy in fetch(pairs, sems):
        copy.wait()


def gather_kernel(sz, in_ref, x_ref, a_ref, b_ref, send_a, send_b, inner_ref):
    band = lax.axis_index("lat")
    start_in, end_in = in_ref[band], in_ref[band + 1]
    below = sz.own + (1 - even("lat")) * sz.halo
    above = sz.own + even("lat") * sz.halo
    step = HALO * sz.cols
    far = (sz.cols - 1) * even("lon")
    member, k = split(column(sz.mp), sz.mrows, sz.members + 1)
    targets = []
    for x in [far, sz.cols - 1 - far] + list(range(1, sz.cols - 1)):
        for side in range(2):
            wanted = 2 * (lax.shift_right_logical(start_in, 1) + k) + side
            own = member * (sz.slots * sz.cols) + (wanted - start_in) * sz.cols + x
            low = below + member * step + (wanted - end_in) * sz.cols + x
            high = above + member * step + (HALO - 1) * sz.cols + x
            t = jnp.where(wanted < start_in, high, jnp.where(wanted < end_in, own, low))
            targets.append(jnp.where((member < sz.members) & (wanted < end_in + HALO), t, -1))
    hot = one_hot(jnp.concatenate(targets, axis=0), sz.own + 2 * sz.halo)
    src = [x_ref[...].reshape(sz.own, sz.packed)]
    src += [r[...].reshape(sz.halo, sz.packed) for r in (a_ref, b_ref)]
    out = dot(hot, jnp.concatenate(src, axis=0)).astype(BF)
    two = 2 * sz.mp
    send_a[...] = out[:two]
    send_b[...] = out[two : 2 * two]
    inner_ref[...] = out[2 * two :]


def merge(sz, columns, gain, bias, weight):
    parts = []
    c = sz.channels
    for level in range(sz.levels):
        for quad in columns:
            at = slice(level * c, level * c + c)
            piece = jnp.concatenate([q[:, at] for q in quad], axis=1)
            parts.append(layer_norm(piece, gain, bias))
    return dot(jnp.concatenate(parts, axis=0).astype(BF), weight)


def finish(sz, block, gain, bias, weight):
    normed = layer_norm(block, gain, bias).astype(BF)
    return dot(normed, weight)


def by_lanes(sz, block, stride, offset):
    rows = [block[(lv * stride + offset) * sz.mp : (lv * stride + offset + 1) * sz.mp] for lv in range(sz.levels)]
    return jnp.concatenate(rows, axis=1)


def halves(sz, block):
    block = block.astype(F32)
    return [block[: sz.mp], block[sz.mp :]]


def row(ref):
    return ref[...].reshape(1, -1)


def inner_kernel(sz, p_ref, dg, db, dw_ref, uw_ref, ug, ub, ow_ref, merged_ref, fine_ref, dw, uw, ow, sems):
    copies = fetch(chunks((dw_ref, dw), CUT) + chunks((uw_ref, uw), CUT) + [(ow_ref, ow)], sems)
    inner = sz.half - 1
    two = 2 * sz.mp
    columns = []
    for i in range(inner):
        quad = []
        for j in range(2):
            quad += halves(sz, p_ref[(2 * i + j) * two : (2 * i + j + 1) * two])
        columns.append(quad)
    finish_all(copies[:CUT])
    coarse = merge(sz, columns, row(dg), row(db), dw[...])
    finish_all(copies[CUT : 2 * CUT])
    widened = dot(coarse.astype(BF), uw[...]).astype(BF).astype(F32)
    copies[-1].wait()
    c = sz.channels
    done = [finish(sz, widened[:, b * c : (b + 1) * c], row(ug), row(ub), ow[...]) for b in range(4)]
    merged = [by_lanes(sz, coarse, inner, i) for i in range(inner)]
    merged_ref[...] = jnp.concatenate(merged, axis=0).astype(BF)
    fine = [by_lanes(sz, done[b], inner, i) for i in range(inner) for b in range(4)]
    fine_ref[...] = jnp.concatenate(fine, axis=0).astype(BF)


def edge_kernel(
    sz, in_ref, out_ref, own_a, own_b, got_a_ref, got_b_ref, dg, db, dw_ref, uw_ref, ug, ub, ow_ref, inm_ref, inf_ref,
    merged_out, fine_out, oa, ob, ga, gb, dw, uw, ow, inm, inf, merged_ref, fine_ref, sems,
):
    copies = fetch(
        [(got_a_ref, ga), (got_b_ref, gb), (own_a, oa), (own_b, ob)]
        + chunks((dw_ref, dw), CUT)
        + chunks((uw_ref, uw), CUT)
        + [(ow_ref, ow), (inm_ref, inm), (inf_ref, inf)],
        sems,
    )
    start_in, end_in, start_out, end_out = bounds_of(in_ref, out_ref)
    is_even = even("lon") == 1
    mp = sz.mp
    c = sz.channels
    first = lax.shift_right_logical(start_in, 1)
    rows = column(sz.members * sz.mslots * sz.half)
    member, rest = split(rows, sz.mslots * sz.half, sz.members)
    slot, j = split(rest, sz.half, sz.mslots)
    t = j * mp + member * sz.mrows + slot + (start_out - first)
    merged_hot = one_hot(jnp.where(slot < end_out - start_out, t, -1), sz.half * mp)
    rows = column(sz.own)
    member, rest = split(rows, sz.slots * sz.cols, sz.members)
    slot, x = split(rest, sz.cols, sz.slots)
    at = start_in + slot
    k = lax.shift_right_logical(at, 1)
    t = (2 * x + (at - 2 * k)) * mp + member * sz.mrows + (k - first)
    fine_hot = one_hot(jnp.where(slot < end_in - start_in, t, -1), 2 * sz.cols * mp)
    for copy in copies[:4]:
        copy.wait()
    a, b, ra, rb = oa[...], ob[...], ga[...], gb[...]
    left = halves(sz, jnp.where(is_even, rb, ra)) + halves(sz, jnp.where(is_even, b, a))
    right = halves(sz, jnp.where(is_even, a, b)) + halves(sz, jnp.where(is_even, ra, rb))
    finish_all(copies[4 : 4 + CUT])
    coarse_left = merge(sz, [left], row(dg), row(db), dw[...])
    coarse_right = merge(sz, [right], row(dg), row(db), dw[...])
    finish_all(copies[4 + CUT : 4 + 2 * CUT])
    wide_left = dot(coarse_left.astype(BF), uw[:, 2 * c :]).astype(BF).astype(F32)
    wide_right = dot(coarse_right.astype(BF), uw[:, : 2 * c]).astype(BF).astype(F32)
    finish_all(copies[4 + 2 * CUT :])
    base = len(copies)
    src = jnp.concatenate([by_lanes(sz, coarse_left, 1, 0), inm[...].astype(F32)], axis=0).astype(BF)
    merged_ref[...] = dot(merged_hot, src).astype(BF).reshape(merged_ref.shape)
    outs = [pltpu.make_async_copy(merged_ref, merged_out, sems.at[base])]
    outs[0].start()
    finer = [
        by_lanes(sz, finish(sz, wide[:, s * c : (s + 1) * c], row(ug), row(ub), ow[...]), 1, 0)
        for wide in (wide_left, wide_right)
        for s in range(2)
    ]
    src = jnp.concatenate(finer[:2] + [inf[...].astype(F32)] + finer[2:], axis=0).astype(BF)
    size = sz.slots * sz.cols
    for m in range(sz.members):
        rows = slice(m * sz.slots, (m + 1) * sz.slots)
        part = dot(fine_hot[m * size : (m + 1) * size], src).astype(BF)
        fine_ref[rows] = part.reshape(sz.slots, sz.cols, sz.packed)
        outs.append(pltpu.make_async_copy(fine_ref.at[rows], fine_out.at[rows], sems.at[base + 1 + m]))
        outs[-1].start()
    finish_all(outs)


ANY = pl.BlockSpec(memory_space=pl.ANY)
SM = pl.BlockSpec(memory_space=pltpu.SMEM)
VM = pl.BlockSpec(memory_space=pltpu.VMEM)


def call(kernel, name, args, specs, outs, out_spec, scratch=()):
    scratch = [pltpu.VMEM(a.shape, a.dtype) for a in scratch]
    sems = {"gather": 0, "rows": 2, "inner": 9, "edge": 32}[name]
    return pl.pallas_call(
        kernel,
        name=name,
        in_specs=specs,
        out_specs=[out_spec] * len(outs),
        out_shape=[jax.ShapeDtypeStruct(s, BF) for s in outs],
        scratch_shapes=scratch + ([pltpu.SemaphoreType.DMA((sems,))] if sems else []),
    )(*args)


def pair_swaps(first, second, axis, ring):
    size = lax.axis_size(axis)
    assert size % 2 == 0
    near = [(i, i ^ 1) for i in range(size)]
    far = [(i, i + 1 if i % 2 else i - 1) for i in range(size)]
    far = [(i, j % size) for i, j in far if ring or 0 <= j < size]
    return lax.ppermute(first, axis, near), lax.ppermute(second, axis, far)


def body(tokens, in_bounds, out_bounds, down_gain, down_bias, down_weight, up_weight, up_gain, up_bias, out_weight):
    sz = Sizes(tokens, down_weight)
    n = sz.members * sz.slots
    p = sz.packed
    part = functools.partial
    params = (down_gain, down_bias, down_weight, up_weight, up_gain, up_bias, out_weight)
    pspecs = [VM, VM, ANY, ANY, VM, VM, ANY]
    weights = [down_weight, up_weight, out_weight]
    lat_shape = (sz.members, HALO, sz.cols, p)
    row_a, row_b = call(part(rows_kernel, sz), "rows", (in_bounds, tokens), [SM, ANY], [lat_shape] * 2, VM)
    row_a, row_b = pair_swaps(row_a, row_b, "lat", False)
    flat = [v.reshape(-1, sz.cols, p) for v in (tokens, row_a, row_b)]
    two = 2 * sz.mp
    inner = sz.half - 1
    send_a, send_b, mid = call(
        part(gather_kernel, sz), "gather", (in_bounds, *flat), [SM, VM, VM, VM], [(two, p), (two, p), (2 * inner * two, p)], VM
    )
    got_a, got_b = pair_swaps(send_a, send_b, "lon", True)
    in_merged, in_fine = call(
        part(inner_kernel, sz), "inner", (mid,) + params, [VM] + pspecs, [(inner * sz.mp, 2 * p), (4 * inner * sz.mp, p)], VM, weights
    )
    merged, fine = call(
        part(edge_kernel, sz),
        "edge",
        (in_bounds, out_bounds, send_a, send_b, got_a, got_b) + params + (in_merged, in_fine),
        [SM, SM, ANY, ANY, ANY, ANY] + pspecs + [ANY, ANY],
        [(sz.members * sz.mslots, sz.half, 2 * p), (n, sz.cols, p)],
        ANY,
        [send_a, send_b, got_a, got_b]
        + weights
        + [in_merged, in_fine]
        + [jax.ShapeDtypeStruct((sz.members * sz.mslots, sz.half, 2 * p), BF), jax.ShapeDtypeStruct((n, sz.cols, p), BF)],
    )
    return (
        merged.reshape(sz.members, sz.mslots, sz.half, 2 * p),
        fine.reshape(sz.members, sz.slots, sz.cols, p),
    )


def solution(mesh):
    return jax.shard_map(
        body,
        mesh=mesh,
        in_specs=(P(None, "lat", "lon", None),) + (P(),) * 9,
        out_specs=(P(None, "lat", "lon", None), P(None, "lat", "lon", None)),
        check_vma=False,
    )
```
